32 devices in a mesh: grp: 1, exp: 32 (over z, y, x, core).
Axes of the slice: x: 2, y: 2, z: 4, core: 2. Of those that a mesh axis runs over, the one named last changes fastest.
Arguments:
- tokens: bfloat16 [512, 2048], P(('grp', 'exp')), may hold values from -6 to 6
- routed_expert_index: int32 [512, 6], P(('grp', 'exp')), may hold values from 0 to 15, all different within a row; in each aligned block of 16 rows (0 to 15, 16 to 31, ...) at most 8 rows name the same one
- routing_gate_weight: float32 [512, 6], P(('grp', 'exp')), may hold values from 0.05 to 0.5
- token_adapter_index: int32 [512], P('grp'), may hold values from 0 to 511
- gate_weight_pieces: bfloat16 [32, 2048, 704], P('exp'), may hold values from -0.125 to 0.125
- up_weight: bfloat16 [32, 2048, 704], P('exp'), may hold values from -0.125 to 0.125
- down_weight: bfloat16 [32, 704, 2048], P('exp'), may hold values from -0.15625 to 0.15625
- adapter_down_matrix: bfloat16 [2048, 8192], P('exp'), may hold values from -0.125 to 0.125
- adapter_up_matrix: bfloat16 [2048, 8192], P('exp'), may hold values from -1.5 to 1.5
Outputs:
- mixed: bfloat16 [512, 2048], P(('grp', 'exp'))
The draws below stay inside these ranges and needn't reach their ends.
Inputs may be any that keep to these rules, and one draw needn't show every extreme that they name: `routed_expert_index`: each token names 6 different experts; among the 16 tokens of one index of exp (aligned blocks of rows) no expert is named more than 8 times.
All inputs are finite; a program needn't handle non-finite values.
Results may differ from the reference program's by a relative error of at most 0.009.
Values may be sent and summed in bfloat16 or wider, within the bound.
A program may use at most 128 MiB of HBM per device.

```python
import math
import jax
import jax.numpy as jnp
import numpy as np
from jax import lax

MODEL_DIM = 2048
FF = 1408
TOP = 6
ADAPTER_RANK = 16
ADAPTER_COUNT = 512
TOKENS_PER_SHARD = 16
EXPERTS = 16
TOKENS = 512
CAP = 8
N_EXP = 32


def plant(entries, key, smallest, largest):
    index_at = [jax.random.randint(jax.random.fold_in(key, axis), (), 0, length) for axis, length in enumerate(entries.shape)]
    main_axis = entries.shape.index(max(entries.shape))
    next_to = index_at[:main_axis] + [(index_at[main_axis] + 1) % entries.shape[main_axis]] + index_at[main_axis + 1:]
    return entries.at[tuple(index_at)].set(smallest).at[tuple(next_to)].set(largest)


def block_levels(own_key, dims, cuts, least, largest):
    def one(axis_at, parts):
        heights = jax.random.uniform(jax.random.fold_in(jax.random.fold_in(own_key, 6), axis_at), (parts,), jnp.float32, least / len(cuts), largest / len(cuts))
        return jnp.repeat(jnp.exp(heights), dims[axis_at] // parts).reshape((-1,) + (1,) * (len(dims) - axis_at - 1))

    factor_of = one(*cuts[0])
    for cut in cuts[1:]:
        factor_of = factor_of * one(*cut)
    return factor_of


def rank_bounds(number_of, slope):
    weights = [(1 << 20) // math.isqrt(grade ** slope) + 1 for grade in range(1, number_of + 1)]
    scale = 1 + sum(weights) // (1 << 30)
    return np.cumsum(np.array([max(1, weight // scale) for weight in weights]))


def skewed_ids(stream_key, extent, number_of, lean):
    listing = rank_bounds(number_of, lean)
    ticket = jax.random.randint(jax.random.fold_in(stream_key, 1), extent, 0, int(listing[number_of - 1]))
    standing = jnp.searchsorted(jnp.asarray(listing, jnp.int32), ticket, side="right")
    return jax.random.permutation(jax.random.fold_in(stream_key, 2), number_of)[standing].astype(jnp.int32)


def assign_block(rng, own, number, rows, number_of, top, most, skew):
    order = jax.random.permutation(rng, number_of)
    heavy_load, ordinary = shares(number_of, rows * top, most, skew, True), shares(number_of, rows * top, most, skew, False)
    places = jnp.arange(number_of)

    def named(tallies, turn):
        used = int((tallies > 0).sum())
        fixed = max(1, used // 4)
        passed = fixed + (places - fixed + turn * (used - fixed)) % max(1, number_of - fixed)
        return jnp.zeros((number_of,), jnp.int32).at[order[jnp.where(places < fixed, places, passed)]].set(jnp.asarray(tallies, jnp.int32))

    tallies = jnp.where(number % 4 == 0, named(heavy_load, number // 4), named(ordinary, number - number // 4 - 1))
    mixed = jax.random.permutation(jax.random.fold_in(own, 3), number_of)
    donor, sink = mixed[0:number_of // 2 * 2:2], mixed[1:number_of // 2 * 2:2]
    room = jnp.minimum(tallies[donor] - 1, most - tallies[sink]) // 2
    room = jnp.where((donor == order[0]) | (sink == order[0]) | (tallies[sink] == 0), 0, jnp.maximum(room, 0))
    passed = jax.random.randint(jax.random.fold_in(own, 4), (number_of // 2,), 0, 1 << 20) % (room + 1)
    tallies = tallies.at[donor].add(-passed).at[sink].add(passed)
    members = jnp.searchsorted(jnp.cumsum(tallies), jnp.arange(rows * top), side="right").astype(jnp.int32)
    table = members.reshape(top, rows).T
    table = table[jax.random.permutation(jax.random.fold_in(own, 1), rows)]
    turn = jax.random.randint(jax.random.fold_in(own, 2), (rows, 1), 0, top)
    return jnp.take_along_axis(table, (jnp.arange(top)[None, :] + turn) % top, axis=1)


def shares(count, total, limit, skew, full):
    loads = [(1 << 20) // math.isqrt(rank ** skew) + 1 for rank in range(1, count + 1)]
    largest = limit if full else min(limit, max(-(-total // count), total * loads[0] // sum(loads)))
    least = 1 if total - largest >= count - 1 else 0
    counts, rest = [largest] + [least] * (count - 1), total - largest - least * (count - 1)
    while rest > 0:
        free = [i for i in range(1, count) if counts[i] < largest] or [i for i in range(1, count) if counts[i] < limit]
        whole, left = sum([loads[i] for i in free]), rest
        for i in free:
            more = min(limit - counts[i], max(1, left * loads[i] // whole), rest)
            counts[i] = counts[i] + more
            rest = rest - more
    return np.array(counts)


def gaussian(stream_key, extent, width, limit, shards=(), kind=jnp.bfloat16):
    drawn = jax.random.normal(stream_key, extent, jnp.float32) * width
    if len(shards) > 0:
        drawn = block_levels(stream_key, extent, shards, -0.22, 0.18) * drawn
    return jnp.clip(drawn, min=-limit, max=limit).astype(kind)


def setup_inputs(seed: int = 0, part: int = 0) -> dict:
    splits = jax.random.split(jax.random.key(seed), 10)
    part_keys = jax.random.split(jax.random.fold_in(splits[9], part), 10)
    tokens = gaussian(part_keys[0], (TOKENS, MODEL_DIM), 1.0, 6.0, ((0, 32),))
    routed_expert_index_keys = jax.random.split(jax.random.fold_in(part_keys[1], 1), TOKENS // TOKENS_PER_SHARD)
    routed_expert_index_turns = jax.random.permutation(jax.random.fold_in(part_keys[1], 3), TOKENS // TOKENS_PER_SHARD)
    routed_expert_index = jax.vmap(lambda own, number: assign_block(jax.random.fold_in(part_keys[1], 2), own, number, TOKENS_PER_SHARD, EXPERTS, TOP, CAP, 2))(routed_expert_index_keys, routed_expert_index_turns).reshape((TOKENS, TOP))
    routing_gate_weight = jnp.clip(jnp.exp(math.log(0.5) - 2.3025851 * jax.random.uniform(part_keys[2], (TOKENS, TOP), jnp.float32) ** block_levels(part_keys[2], (TOKENS, TOP), ((0, 32),), -0.2, 0.2)), 0.05, 0.5)
    token_adapter_index = plant(skewed_ids(part_keys[3], (TOKENS,), ADAPTER_COUNT, 2), jax.random.fold_in(part_keys[3], 3), 0, ADAPTER_COUNT - 1).astype(jnp.int32)
    gate_weight_pieces = gaussian(splits[4], (2 * EXPERTS, MODEL_DIM, FF // 2), MODEL_DIM ** -0.5, 0.125, ((0, 32),))
    up_weight = gaussian(splits[5], (2 * EXPERTS, MODEL_DIM, FF // 2), MODEL_DIM ** -0.5, 0.125, ((0, 32),))
    down_weight = gaussian(splits[6], (2 * EXPERTS, FF // 2, MODEL_DIM), FF ** -0.5, 0.15625, ((0, 32),))
    adapter_down_matrix = gaussian(splits[7], (MODEL_DIM, ADAPTER_COUNT * ADAPTER_RANK), MODEL_DIM ** -0.5, 0.125, ((0, 32),))
    adapter_up_matrix = gaussian(splits[8], (MODEL_DIM, ADAPTER_COUNT * ADAPTER_RANK), ADAPTER_RANK ** -0.5, 1.5, ((0, 32),))
    return dict(tokens=tokens, routed_expert_index=routed_expert_index, routing_gate_weight=routing_gate_weight, token_adapter_index=token_adapter_index, gate_weight_pieces=gate_weight_pieces, up_weight=up_weight, down_weight=down_weight, adapter_down_matrix=adapter_down_matrix, adapter_up_matrix=adapter_up_matrix)


def reference(tokens, routed_expert_index, routing_gate_weight, token_adapter_index, gate_weight_pieces, up_weight, down_weight, adapter_down_matrix, adapter_up_matrix):
    flat_ids = routed_expert_index.reshape(N_EXP, TOKENS_PER_SHARD * TOP)
    one_hot = (flat_ids[:, :, None] == jnp.arange(EXPERTS, dtype=jnp.int32)[None, None, :]).astype(jnp.int32)
    counted = jnp.cumsum(one_hot, axis=1)
    position = jnp.sum(one_hot * counted, axis=2) - 1
    block_ids = jnp.arange(N_EXP, dtype=jnp.int32)[:, None]
    column = (block_ids * CAP + position).reshape(-1).astype(jnp.int32)
    expert_col = flat_ids.reshape(-1).astype(jnp.int32)
    token_col = (jnp.arange(TOKENS * TOP, dtype=jnp.int32) // TOP).astype(jnp.int32)
    row_table = jnp.full((EXPERTS, N_EXP * CAP), TOKENS, jnp.int32).at[expert_col, column].set(token_col)
    row_gates = jnp.zeros((EXPERTS, N_EXP * CAP), jnp.float32).at[expert_col, column].set(routing_gate_weight.reshape(-1))
    padded = jnp.concatenate([tokens, jnp.zeros((1, MODEL_DIM), tokens.dtype)], axis=0)

    def one_expert(summed, expert):
        rows_index = row_table[expert]
        row_block = padded[rows_index]
        output = jnp.zeros((row_block.shape[0], MODEL_DIM), jnp.float32)
        for which in range(2):
            slab_index = 2 * expert + which
            gate_act = jnp.dot(row_block, gate_weight_pieces[slab_index], preferred_element_type=jnp.float32)
            up_act = jnp.dot(row_block, up_weight[slab_index], preferred_element_type=jnp.float32)
            hidden = (jax.nn.silu(gate_act) * up_act).astype(jnp.bfloat16)
            output = output + jnp.dot(hidden, down_weight[slab_index], preferred_element_type=jnp.float32)
        summed = summed.at[rows_index].add(row_gates[expert][:, None] * output)
        return summed, None

    start = jnp.zeros((TOKENS + 1, MODEL_DIM), jnp.float32)
    routed, _ = lax.scan(one_expert, start, jnp.arange(EXPERTS, dtype=jnp.int32))
    routed = routed[:TOKENS]

    down_adapter_matrix = adapter_down_matrix.reshape(MODEL_DIM, ADAPTER_COUNT, ADAPTER_RANK)
    up_adapter_matrix = adapter_up_matrix.reshape(MODEL_DIM, ADAPTER_COUNT, ADAPTER_RANK)

    def adapter_block_rows(input_rows):
        x_block, id_block = input_rows
        down_selected = down_adapter_matrix[:, id_block, :].astype(jnp.float32)
        low_rank = jnp.einsum("td,dtr->tr", x_block.astype(jnp.float32), down_selected).astype(jnp.bfloat16)
        up_selected = up_adapter_matrix[:, id_block, :].astype(jnp.float32)
        return jnp.einsum("tr,dtr->td", low_rank.astype(jnp.float32), up_selected).astype(jnp.bfloat16)

    lowrank_delta = lax.map(adapter_block_rows, (tokens.reshape(N_EXP, TOKENS_PER_SHARD, MODEL_DIM), token_adapter_index.reshape(N_EXP, TOKENS_PER_SHARD)))
    lowrank_delta = lowrank_delta.reshape(TOKENS, MODEL_DIM)
    return (routed + lowrank_delta.astype(jnp.float32)).astype(jnp.bfloat16)
```

```python
import functools

import jax
import jax.numpy as jnp
from jax import lax
from jax.experimental import pallas as pl
from jax.experimental.pallas import tpu as pltpu
from jax.sharding import PartitionSpec as P

RANK = 16
LANES = 128
BF16 = jnp.bfloat16
F32 = jnp.float32
MESH = pl.DeviceIdType.MESH


def kernel(
    chips, cap, top, x_ref, idx_ref, gate_ref, aid_ref, wg_hbm, wu_hbm, wd_hbm, adn_hbm, aup_hbm, out_ref,
    wg, wu, wd, adn, aup, col, disp, recv_a, recv_b, xs, hid, y_own, sib_send, sib_recv,
    rs_send, rs_recv, ag, cor_send, cor_recv, ret_send, ret_recv, low,
    w_sem, adl_sem, ad_s, ad_r, col_s, col_r, disp_s, disp_r, fwd_s, fwd_r, rs_s, rs_r,
    ag_s, ag_r, cor_s, cor_r, ret_s, ret_r, sib_s, sib_r,
):
    me = lax.axis_index("exp")
    q = lax.div(me, 2)
    c = lax.rem(me, 2)
    sib = me + 1 - 2 * c
    rows, width = x_ref.shape
    feats = adn_hbm.shape[0]
    bank = adn_hbm.shape[1]
    group = chips * rows
    slots = chips * cap
    off = pl.multiple_of(lax.rem(me * feats, LANES), feats)

    def remote(src, dst, ss, rs, dev):
        return pltpu.make_async_remote_copy(
            src_ref=src, dst_ref=dst, send_sem=ss, recv_sem=rs, device_id={"exp": dev}, device_id_type=MESH
        )

    def peer(r):
        return lax.rem(q + r, chips)

    def source(r):
        return lax.rem(q + chips - r, chips)

    def others(fn):
        def step(r, carry):
            fn(r)
            return carry

        lax.fori_loop(1, chips, step, 0)

    barrier = pltpu.get_barrier_semaphore()
    if 2 * feats < LANES:
        adn[...] = jnp.zeros_like(adn)
        aup[...] = jnp.zeros_like(aup)
    others(lambda r: pl.semaphore_signal(barrier, inc=1, device_id={"exp": 2 * peer(r) + c}, device_id_type=MESH))
    pl.semaphore_signal(barrier, inc=1, device_id={"exp": sib}, device_id_type=MESH)

    own_rows = pl.ds(off, feats)
    local = [
        pltpu.make_async_copy(adn_hbm, adn.at[own_rows], adl_sem.at[0]),
        pltpu.make_async_copy(wg_hbm.at[0], wg, w_sem.at[0]),
        pltpu.make_async_copy(wu_hbm.at[0], wu, w_sem.at[1]),
        pltpu.make_async_copy(aup_hbm, aup.at[own_rows], adl_sem.at[1]),
        pltpu.make_async_copy(wd_hbm.at[0], wd, w_sem.at[2]),
    ]
    for cp in local:
        cp.start()

    lane = lax.broadcasted_iota(jnp.int32, (rows, slots), 1)
    lane_e = lax.div(lane, cap)
    chosen = jnp.zeros((rows, slots), F32)
    weight = jnp.zeros((rows, slots), F32)
    for k in range(top):
        hit = idx_ref[:, k : k + 1] == lane_e
        chosen = chosen + jnp.where(hit, 1.0, 0.0)
        weight = weight + jnp.where(hit, gate_ref[:, k : k + 1], 0.0)
    lower = jnp.where(
        lax.broadcasted_iota(jnp.int32, (rows, rows), 1) < lax.broadcasted_iota(jnp.int32, (rows, rows), 0), 1.0, 0.0
    )
    rank_of = jnp.dot(lower.astype(BF16), chosen.astype(BF16), preferred_element_type=F32)
    slot_p = lax.rem(lane, cap).astype(F32)
    pick = jnp.where((chosen > 0.5) & (rank_of == slot_p), 1.0, 0.0)
    combine = pick * weight
    packed = jnp.dot(pick.T.astype(BF16), x_ref[...], preferred_element_type=F32)
    disp[...] = packed.reshape(chips, cap, width).astype(BF16)
    recv_a[pl.ds(q, 1)] = disp[pl.ds(q, 1)]

    def lanes_of(chip):
        return pl.ds(pl.multiple_of(lax.div(chip * 2 * feats, LANES) * LANES, LANES), LANES)

    col[pl.ds(q, 1)] = x_ref[:, lanes_of(q)].reshape(1, rows, LANES)

    pl.semaphore_wait(barrier, chips)

    def col_copy(to, slot):
        return remote(x_ref.at[:, lanes_of(to)], col.at[slot], col_s.at[to], col_r.at[slot], 2 * to + c)

    def disp_copy(to, slot):
        return remote(disp.at[to], recv_a.at[slot], disp_s.at[to], disp_r.at[slot], 2 * to + c)

    def fwd_copy(block):
        return remote(recv_a.at[block], recv_b.at[block], fwd_s.at[block], fwd_r.at[block], sib)

    def rs_copy(to, slot):
        return remote(rs_send.at[to], rs_recv.at[slot], rs_s.at[to], rs_r.at[slot], 2 * to + c)

    def ag_copy(to, slot):
        return remote(low, ag.at[slot], ag_s.at[to], ag_r.at[slot], 2 * to + c)

    def cor_copy(to, slot):
        return remote(cor_send.at[to], cor_recv.at[slot], cor_s.at[to], cor_r.at[slot], 2 * to + c)

    def ret_copy(to, slot):
        return remote(ret_send.at[to], ret_recv.at[slot], ret_s.at[to], ret_r.at[slot], 2 * to + c)

    others(lambda r: col_copy(peer(r), q).start())
    adn_copy = remote(adn_hbm, adn.at[own_rows], ad_s.at[0], ad_r.at[0], sib)
    aup_copy = remote(aup_hbm, aup.at[own_rows], ad_s.at[1], ad_r.at[1], sib)
    adn_copy.start()
    others(lambda r: disp_copy(peer(r), q).start())
    aup_copy.start()
    fwd_copy(q).start()

    part = lax.broadcasted_iota(jnp.int32, (chips, rows, 2 * rows), 2)
    row = lax.broadcasted_iota(jnp.int32, (chips, rows, 2 * rows), 1)
    spread = jnp.broadcast_to(aid_ref[...].astype(F32)[:, None, :], (chips, rows, 2 * rows))
    ids = jnp.sum(jnp.where(part == row + c * rows, spread, 0.0), axis=2, keepdims=True)
    ids = jnp.broadcast_to(ids, (chips, rows, LANES)).reshape(group, LANES).astype(jnp.int32)
    per = LANES // RANK
    id_hi = lax.div(ids, per)
    id_lo = ids - id_hi * per
    lane_g = lax.broadcasted_iota(jnp.int32, (group, LANES), 1)
    keep = lax.div(lane_g, RANK) == id_lo

    others(lambda r: col_copy(q, source(r)).wait_recv())
    local[0].wait()
    adn_copy.wait_recv()
    cols = col[...].reshape(group, LANES)
    span = 512
    sub = span // LANES

    def down_step(i, acc):
        at = pl.multiple_of(i * span, span)
        h = jnp.dot(cols, adn[:, pl.ds(at, span)], preferred_element_type=F32)
        for s in range(sub):
            acc = jnp.where(id_hi == i * sub + s, h[:, s * LANES : (s + 1) * LANES], acc)
        return acc

    terms = lax.fori_loop(0, bank // span, down_step, jnp.zeros((group, LANES), F32))
    terms = jnp.where(keep, terms, 0.0).astype(BF16)
    fi = lax.broadcasted_iota(jnp.int32, (LANES, LANES), 0)
    fj = lax.broadcasted_iota(jnp.int32, (LANES, LANES), 1)
    fold = jnp.where(lax.rem(fi, RANK) == lax.rem(fj, RANK), 1.0, 0.0).astype(BF16)
    folded = jnp.dot(terms, fold, preferred_element_type=F32).astype(BF16)
    rs_send[...] = folded.reshape(chips, rows, LANES)
    rs_recv[pl.ds(q, 1)] = rs_send[pl.ds(q, 1)]
    others(lambda r: rs_copy(peer(r), q).start())

    def forward(r):
        disp_copy(q, source(r)).wait_recv()
        fwd_copy(source(r)).start()

    others(forward)

    others(lambda r: rs_copy(q, source(r)).wait_recv())
    low[...] = jnp.sum(rs_recv[...].astype(F32), axis=0).astype(BF16)
    ag[pl.ds(q, 1)] = low[...].reshape(1, rows, LANES)
    others(lambda r: ag_copy(peer(r), q).start())

    ksplit = 512
    nsplit = 512
    half = wd.shape[0]

    def load_rows(ref):
        xs[...] = ref[...].astype(F32).reshape(slots, width).astype(BF16)

    def hidden():
        def step(i, accs):
            at = pl.multiple_of(i * ksplit, ksplit)
            xk = xs[:, pl.ds(at, ksplit)]
            return (
                accs[0] + jnp.dot(xk, wg[pl.ds(at, ksplit), :], preferred_element_type=F32),
                accs[1] + jnp.dot(xk, wu[pl.ds(at, ksplit), :], preferred_element_type=F32),
            )

        zero = jnp.zeros((slots, half), F32)
        g, u = lax.fori_loop(0, width // ksplit, step, (zero, zero))
        hid[...] = (g / (1.0 + jnp.exp(-g)) * u).astype(BF16)

    load_rows(recv_a)
    local[1].wait()
    local[2].wait()
    hidden()
    local[4].wait()

    def own_step(i, carry):
        at = pl.ds(pl.multiple_of(i * nsplit, nsplit), nsplit)
        y_own[:, at] = jnp.dot(hid[...], wd[:, at], preferred_element_type=F32)
        return carry

    lax.fori_loop(0, width // nsplit, own_step, 0)

    fwd_in = lambda block: fwd_copy(block).wait_recv()
    fwd_in(q)
    others(lambda r: fwd_in(source(r)))
    load_rows(recv_b)
    hidden()

    def sib_step(i, carry):
        at = pl.ds(pl.multiple_of(i * nsplit, nsplit), nsplit)
        y = jnp.dot(hid[...], wd[:, at], preferred_element_type=F32)
        sib_send[:, :, at] = y.reshape(chips, cap, nsplit).astype(BF16)
        return carry

    lax.fori_loop(0, width // nsplit, sib_step, 0)
    sib_copy = remote(sib_send, sib_recv, sib_s.at[0], sib_r.at[0], sib)
    sib_copy.start()

    others(lambda r: ag_copy(q, source(r)).wait_recv())
    local[3].wait()
    aup_copy.wait_recv()
    ranks = jnp.where(keep, ag[...].reshape(group, LANES).astype(F32), 0.0)

    def up_step(i, acc):
        at = pl.multiple_of(i * span, span)
        wide = jnp.concatenate([jnp.where(id_hi == i * sub + s, ranks, 0.0).astype(BF16) for s in range(sub)], axis=1)
        return acc + lax.dot_general(
            wide, aup[:, pl.ds(at, span)], (((1,), (1,)), ((), ())), preferred_element_type=F32
        )

    corr = lax.fori_loop(0, bank // span, up_step, jnp.zeros((group, LANES), F32))
    cor_send[...] = corr.astype(BF16).reshape(chips, rows, LANES)
    cor_recv[pl.ds(q, 1)] = cor_send[pl.ds(q, 1)]
    others(lambda r: cor_copy(peer(r), q).start())

    sib_copy.wait_recv()
    ret_send[...] = (y_own[...].reshape(chips, cap, width) + sib_recv[...].astype(F32)).astype(BF16)
    ret_recv[pl.ds(q, 1)] = ret_send[pl.ds(q, 1)]
    others(lambda r: ret_copy(peer(r), q).start())

    others(lambda r: cor_copy(q, source(r)).wait_recv())
    others(lambda r: ret_copy(q, source(r)).wait_recv())
    back = ret_recv[...].astype(F32).reshape(slots, width).astype(BF16)
    c_hi = combine.astype(BF16)
    c_lo = (combine - c_hi.astype(F32)).astype(BF16)
    routed = jnp.dot(c_hi, back, preferred_element_type=F32) + jnp.dot(c_lo, back, preferred_element_type=F32)
    share = LANES // (2 * feats)
    for j in range(width // LANES):
        delta = cor_recv[j * share].astype(F32)
        for s in range(1, share):
            delta = delta + cor_recv[j * share + s].astype(F32)
        at = slice(j * LANES, (j + 1) * LANES)
        out_ref[:, at] = (routed[:, at] + delta).astype(BF16)

    adn_copy.wait_send()
    aup_copy.wait_send()
    sib_copy.wait_send()
    fwd_copy(q).wait_send()

    def drain(r):
        to = peer(r)
        for cp in (col_copy, disp_copy, rs_copy, ag_copy, cor_copy, ret_copy):
            cp(to, q).wait_send()
        fwd_copy(source(r)).wait_send()

    others(drain)


def per_device(tokens, idx, gates, aid, wg, wu, wd, adn, aup):
    devices = lax.axis_size("exp")
    chips = devices // 2
    rows, width = tokens.shape
    top = idx.shape[1]
    half = wd.shape[1]
    feats, bank = adn.shape
    need = 2 * (rows * top // devices + 1)
    cap = -(-need // 8) * 8
    slots = chips * cap
    group = chips * rows
    blocks = lambda *s: pltpu.VMEM(s, BF16)
    sems = lambda n: pltpu.SemaphoreType.DMA((n,))
    vm = pl.BlockSpec(memory_space=pltpu.VMEM)
    hbm = pl.BlockSpec(memory_space=pl.ANY)
    return pl.pallas_call(
        functools.partial(kernel, chips, cap, top),
        out_shape=jax.ShapeDtypeStruct((rows, width), BF16),
        in_specs=[vm, vm, vm, vm, hbm, hbm, hbm, hbm, hbm],
        out_specs=vm,
        scratch_shapes=[
            blocks(width, half), blocks(width, half), blocks(half, width),
            blocks(LANES, bank), blocks(LANES, bank),
            blocks(chips, rows, LANES),
            blocks(chips, cap, width), blocks(chips, cap, width), blocks(chips, cap, width),
            blocks(slots, width), blocks(slots, half), pltpu.VMEM((slots, width), F32),
            blocks(chips, cap, width), blocks(chips, cap, width),
            blocks(chips, rows, LANES), blocks(chips, rows, LANES), blocks(chips, rows, LANES),
            blocks(chips, rows, LANES), blocks(chips, rows, LANES),
            blocks(chips, cap, width), blocks(chips, cap, width), blocks(rows, LANES),
            sems(3), sems(2), sems(2), sems(2),
            *[sems(chips) for _ in range(14)],
            sems(1), sems(1),
        ],
        compiler_params=pltpu.CompilerParams(
            collective_id=0, has_side_effects=True, vmem_limit_bytes=60 * 1024 * 1024
        ),
    )(tokens, idx, gates, aid.reshape(chips, 2 * rows), wg, wu, wd, adn, aup)


def solution(mesh):
    placed = (
        P(("grp", "exp"), None),
        P(("grp", "exp"), None),
        P(("grp", "exp"), None),
        P("grp"),
        P("exp", None, None),
        P("exp", None, None),
        P("exp", None, None),
        P("exp", None),
        P("exp", None),
    )
    return jax.shard_map(
        per_device, mesh=mesh, in_specs=placed, out_specs=P(("grp", "exp"), None), check_vma=False
    )
```

```python
import functools

import jax
import jax.numpy as jnp
from jax import lax
from jax.experimental import pallas as pl
from jax.experimental.pallas import tpu as pltpu
from jax.sharding import PartitionSpec as P

RANK = 16
LANES = 128
BF16 = jnp.bfloat16
F32 = jnp.float32
MESH = pl.DeviceIdType.MESH


def dot_nt(a, b):
    return lax.dot_general(a, b, (((1,), (1,)), ((), ())), preferred_element_type=F32)


def kernel(
    chips, cap, top, x_ref, idx_ref, gate_ref, aid_ref, wg_hbm, wu_hbm, wd_hbm, adn_hbm, aup_hbm, out_ref,
    wg, wu, wd, adn, aup, col, disp, recv_a, recv_b, xs, hid, y_own, sib_send, sib_recv,
    rs_send, rs_recv, ag, cor_send, cor_recv, ret_send, ret_recv, low,
    w_sem, adl_sem, ad_s, ad_r, col_s, col_r, disp_s, disp_r, fwd_s, fwd_r, rs_s, rs_r,
    ag_s, ag_r, cor_s, cor_r, ret_s, ret_r, sib_s, sib_r,
):
    me = lax.axis_index("exp")
    q = lax.div(me, 2)
    c = lax.rem(me, 2)
    sib = me + 1 - 2 * c
    rows, width = x_ref.shape
    feats = adn_hbm.shape[0]
    bank = adn_hbm.shape[1]
    group = chips * rows
    slots = chips * cap
    parts, wide_n = y_own.shape[0], y_own.shape[2]
    off = pl.multiple_of(lax.rem(me * feats, LANES), feats)

    def remote(src, dst, ss, rs, dev):
        return pltpu.make_async_remote_copy(
            src_ref=src, dst_ref=dst, send_sem=ss, recv_sem=rs, device_id={"exp": dev}, device_id_type=MESH
        )

    def peer(r):
        return lax.rem(q + r, chips)

    def source(r):
        return lax.rem(q + chips - r, chips)

    def others(fn, first=1, last=chips):
        def step(r, carry):
            fn(r)
            return carry

        lax.fori_loop(first, last, step, 0)

    barrier = pltpu.get_barrier_semaphore()
    if 2 * feats < LANES:
        adn[...] = jnp.zeros_like(adn)
        aup[...] = jnp.zeros_like(aup)
    others(lambda r: pl.semaphore_signal(barrier, inc=1, device_id={"exp": 2 * peer(r) + c}, device_id_type=MESH))
    pl.semaphore_signal(barrier, inc=1, device_id={"exp": sib}, device_id_type=MESH)

    own_rows = pl.ds(off, feats)
    local = [
        pltpu.make_async_copy(adn_hbm, adn.at[own_rows], adl_sem.at[0]),
        pltpu.make_async_copy(wg_hbm.at[0], wg, w_sem.at[0]),
        pltpu.make_async_copy(wu_hbm.at[0], wu, w_sem.at[1]),
        pltpu.make_async_copy(aup_hbm, aup.at[own_rows], adl_sem.at[1]),
        pltpu.make_async_copy(wd_hbm.at[0], wd, w_sem.at[2]),
    ]
    for cp in local:
        cp.start()

    slot = lax.broadcasted_iota(jnp.int32, (slots, rows), 0)
    slot_e = lax.div(slot, cap)
    chosen = jnp.zeros((slots, rows), F32)
    weight = jnp.zeros((slots, rows), F32)
    for k in range(top):
        hit = idx_ref[k : k + 1, :] == slot_e
        chosen = chosen + jnp.where(hit, 1.0, 0.0)
        weight = weight + jnp.where(hit, gate_ref[k : k + 1, :], 0.0)
    earlier = jnp.where(
        lax.broadcasted_iota(jnp.int32, (rows, rows), 0) < lax.broadcasted_iota(jnp.int32, (rows, rows), 1), 1.0, 0.0
    )
    rank_of = jnp.dot(chosen.astype(BF16), earlier.astype(BF16), preferred_element_type=F32)
    slot_p = lax.rem(slot, cap).astype(F32)
    pick = jnp.where((chosen > 0.5) & (rank_of == slot_p), 1.0, 0.0)
    packed = jnp.dot(pick.astype(BF16), x_ref[...], preferred_element_type=F32)
    disp[...] = packed.reshape(chips, cap, width).astype(BF16)
    recv_a[pl.ds(q, 1)] = disp[pl.ds(q, 1)]

    def lanes_of(chip):
        return pl.ds(pl.multiple_of(lax.div(chip * 2 * feats, LANES) * LANES, LANES), LANES)

    col[pl.ds(q, 1)] = x_ref[:, lanes_of(q)].reshape(1, rows, LANES)

    pl.semaphore_wait(barrier, chips)

    def col_copy(to, slot):
        return remote(x_ref.at[:, lanes_of(to)], col.at[slot], col_s.at[to], col_r.at[slot], 2 * to + c)

    def disp_copy(to, slot):
        return remote(disp.at[to], recv_a.at[slot], disp_s.at[to], disp_r.at[slot], 2 * to + c)

    def fwd_copy(block):
        return remote(recv_a.at[block], recv_b.at[block], fwd_s.at[block], fwd_r.at[block], sib)

    def rs_copy(to, slot):
        return remote(rs_send.at[to], rs_recv.at[slot], rs_s.at[to], rs_r.at[slot], 2 * to + c)

    def ag_copy(to, slot):
        return remote(low, ag.at[slot], ag_s.at[to], ag_r.at[slot], 2 * to + c)

    def cor_copy(to, slot):
        return remote(cor_send.at[to], cor_recv.at[slot], cor_s.at[to], cor_r.at[slot], 2 * to + c)

    def ret_copy(j, to, slot):
        return remote(
            ret_send.at[j, to], ret_recv.at[j, slot], ret_s.at[j * chips + to], ret_r.at[j * chips + slot], 2 * to + c
        )

    def sib_copy(j):
        return remote(sib_send.at[j], sib_recv.at[j], sib_s.at[j], sib_r.at[j], sib)

    others(lambda r: col_copy(peer(r), q).start())
    adn_copy = remote(adn_hbm, adn.at[own_rows], ad_s.at[0], ad_r.at[0], sib)
    aup_copy = remote(aup_hbm, aup.at[own_rows], ad_s.at[1], ad_r.at[1], sib)
    adn_copy.start()
    early = 1 + (chips - 1) * 5 // 8
    others(lambda r: disp_copy(peer(r), q).start(), 1, early)
    aup_copy.start()
    fwd_copy(q).start()

    piece = 8 * LANES // (2 * rows)
    ids = []
    for first in range(0, chips, piece):
        n = min(piece, chips - first)
        part = lax.broadcasted_iota(jnp.int32, (n * rows, n * 2 * rows), 1)
        row = lax.broadcasted_iota(jnp.int32, (n * rows, n * 2 * rows), 0)
        here = lax.div(row, rows) * (2 * rows) + lax.rem(row, rows) + c * rows
        values = aid_ref[:, first * 2 * rows : (first + n) * 2 * rows].astype(F32)
        ids.append(jnp.sum(jnp.where(part == here, values, 0.0), axis=1, keepdims=True))
    ids = jnp.concatenate(ids, axis=0) if len(ids) > 1 else ids[0]
    ids = jnp.broadcast_to(ids, (group, LANES)).astype(jnp.int32)
    per = LANES // RANK
    id_hi = lax.div(ids, per)
    id_lo = ids - id_hi * per
    lane_g = lax.broadcasted_iota(jnp.int32, (group, LANES), 1)
    keep = lax.div(lane_g, RANK) == id_lo

    others(lambda r: col_copy(q, source(r)).wait_recv())
    local[0].wait()
    adn_copy.wait_recv()
    cols = col[...].reshape(group, LANES)
    span = 512
    sub = span // LANES

    def down_step(i, acc):
        at = pl.multiple_of(i * span, span)
        h = jnp.dot(cols, adn[:, pl.ds(at, span)], preferred_element_type=F32)
        for s in range(sub):
            acc = jnp.where(id_hi == i * sub + s, h[:, s * LANES : (s + 1) * LANES], acc)
        return acc

    terms = lax.fori_loop(0, bank // span, down_step, jnp.zeros((group, LANES), F32))
    terms = jnp.where(keep, terms, 0.0).astype(BF16)
    fi = lax.broadcasted_iota(jnp.int32, (LANES, LANES), 0)
    fj = lax.broadcasted_iota(jnp.int32, (LANES, LANES), 1)
    fold = jnp.where(lax.rem(fi, RANK) == lax.rem(fj, RANK), 1.0, 0.0).astype(BF16)
    turn = lax.div(lane_g, RANK) == lax.rem(lax.broadcasted_iota(jnp.int32, (group, LANES), 0), per)
    folded = jnp.where(turn, jnp.dot(terms, fold, preferred_element_type=F32), 0.0)
    rs_send[...] = jnp.sum(folded.reshape(group // per, per, LANES), axis=1).reshape(chips, rows // per, LANES)
    rs_recv[pl.ds(q, 1)] = rs_send[pl.ds(q, 1)]
    others(lambda r: rs_copy(peer(r), q).start())

    others(lambda r: disp_copy(peer(r), q).start(), early, chips)

    def forward(r):
        disp_copy(q, source(r)).wait_recv()
        fwd_copy(source(r)).start()

    others(forward, 1, early)
    others(lambda r: rs_copy(q, source(r)).wait_recv())
    low[...] = jnp.sum(rs_recv[...], axis=0).astype(BF16).astype(F32)
    ag[pl.ds(q, 1)] = low[...].reshape(1, rows // per, LANES)
    others(lambda r: ag_copy(peer(r), q).start())
    others(forward, early, chips)

    half = wd.shape[0]
    xs[:slots] = recv_a[...].astype(F32).reshape(slots, width).astype(BF16)
    local[1].wait()
    local[2].wait()
    local[4].wait()
    fwd_copy(q).wait_recv()
    others(lambda r: fwd_copy(source(r)).wait_recv())
    xs[slots:] = recv_b[...].astype(F32).reshape(slots, width).astype(BF16)
    cut = -(-half // (2 * LANES)) * LANES
    for a, b in ((0, cut), (cut, half)):
        g = dot_nt(wg[a:b], xs[...])
        u = dot_nt(wu[a:b], xs[...])
        hid[:, a:b] = (g / (1.0 + jnp.exp(-g)) * u).T.astype(BF16)

    def finish(j):
        sib_copy(j).wait_recv()
        ret_send[j] = (y_own[j].reshape(chips, cap, wide_n) + sib_recv[j].astype(F32)).astype(BF16)
        ret_recv[j, pl.ds(q, 1)] = ret_send[j, pl.ds(q, 1)]
        others(lambda r: ret_copy(j, peer(r), q).start())

    for j in range(parts):
        y = jnp.dot(hid[...], wd[:, j * wide_n : (j + 1) * wide_n], preferred_element_type=F32)
        sib_send[j] = y[slots:].reshape(chips, cap, wide_n).astype(BF16)
        sib_copy(j).start()
        y_own[j] = y[:slots]
        if j > 0:
            finish(j - 1)
    finish(parts - 1)

    others(lambda r: ag_copy(q, source(r)).wait_recv())
    local[3].wait()
    aup_copy.wait_recv()
    ranks = jnp.broadcast_to(ag[...].reshape(group // per, 1, LANES), (group // per, per, LANES)).reshape(group, LANES)
    ranks = jnp.where(turn, ranks, 0.0).astype(BF16)
    ranks = jnp.where(keep, jnp.dot(ranks, fold, preferred_element_type=F32), 0.0)

    def up_step(i, acc):
        at = pl.multiple_of(i * span, span)
        wide = jnp.concatenate([jnp.where(id_hi == i * sub + s, ranks, 0.0).astype(BF16) for s in range(sub)], axis=1)
        return acc + dot_nt(wide, aup[:, pl.ds(at, span)])

    corr = lax.fori_loop(0, bank // span, up_step, jnp.zeros((group, LANES), F32))
    cor_send[...] = corr.astype(BF16).reshape(chips, rows, LANES)
    cor_recv[pl.ds(q, 1)] = cor_send[pl.ds(q, 1)]
    others(lambda r: cor_copy(peer(r), q).start())

    others(lambda r: cor_copy(q, source(r)).wait_recv())
    combine = (pick * weight).T
    c_hi = combine.astype(BF16)
    c_lo = (combine - c_hi.astype(F32)).astype(BF16)
    share = LANES // (2 * feats)
    for j in range(parts):
        others(lambda r: ret_copy(j, q, source(r)).wait_recv())
        back = ret_recv[j].astype(F32).reshape(slots, wide_n).astype(BF16)
        routed = jnp.dot(c_hi, back, preferred_element_type=F32) + jnp.dot(c_lo, back, preferred_element_type=F32)
        for i in range(wide_n // LANES):
            first = (j * wide_n // LANES + i) * share
            delta = cor_recv[first].astype(F32)
            for s in range(1, share):
                delta = delta + cor_recv[first + s].astype(F32)
            out_ref[:, j * wide_n + i * LANES : j * wide_n + (i + 1) * LANES] = (
                routed[:, i * LANES : (i + 1) * LANES] + delta
            ).astype(BF16)

    adn_copy.wait_send()
    aup_copy.wait_send()
    for j in range(parts):
        sib_copy(j).wait_send()
    fwd_copy(q).wait_send()

    def drain(r):
        to = peer(r)
        for cp in (col_copy, disp_copy, rs_copy, ag_copy, cor_copy):
            cp(to, q).wait_send()
        for j in range(parts):
            ret_copy(j, to, q).wait_send()
        fwd_copy(source(r)).wait_send()

    others(drain)


def per_device(tokens, idx, gates, aid, wg, wu, wd, adn, aup):
    devices = lax.axis_size("exp")
    chips = devices // 2
    rows, width = tokens.shape
    top = idx.shape[1]
    half = wd.shape[1]
    feats, bank = adn.shape
    need = 2 * (rows * top // devices + 1)
    cap = -(-need // 8) * 8
    slots = chips * cap
    short = rows * RANK // LANES
    parts = 4
    wide_n = width // parts
    blocks = lambda *s: pltpu.VMEM(s, BF16)
    sems = lambda n: pltpu.SemaphoreType.DMA((n,))
    vm = pl.BlockSpec(memory_space=pltpu.VMEM)
    hbm = pl.BlockSpec(memory_space=pl.ANY)
    return pl.pallas_call(
        functools.partial(kernel, chips, cap, top),
        out_shape=jax.ShapeDtypeStruct((rows, width), BF16),
        in_specs=[vm, vm, vm, vm, hbm, hbm, hbm, hbm, hbm],
        out_specs=vm,
        scratch_shapes=[
            blocks(half, width), blocks(half, width), blocks(half, width),
            blocks(LANES, bank), blocks(LANES, bank),
            blocks(chips, rows, LANES),
            blocks(chips, cap, width), blocks(chips, cap, width), blocks(chips, cap, width),
            blocks(2 * slots, width), blocks(2 * slots, half), pltpu.VMEM((parts, slots, wide_n), F32),
            blocks(parts, chips, cap, wide_n), blocks(parts, chips, cap, wide_n),
            pltpu.VMEM((chips, short, LANES), F32), pltpu.VMEM((chips, short, LANES), F32),
            pltpu.VMEM((chips, short, LANES), F32),
            blocks(chips, rows, LANES), blocks(chips, rows, LANES),
            blocks(parts, chips, cap, wide_n), blocks(parts, chips, cap, wide_n), pltpu.VMEM((short, LANES), F32),
            sems(3), sems(2), sems(2), sems(2),
            *[sems(chips) for _ in range(12)],
            sems(parts * chips), sems(parts * chips), sems(parts), sems(parts),
        ],
        compiler_params=pltpu.CompilerParams(
            collective_id=0, has_side_effects=True, vmem_limit_bytes=60 * 1024 * 1024
        ),
    )(tokens, idx.T, gates.T, aid.reshape(1, -1), wg.swapaxes(1, 2), wu.swapaxes(1, 2), wd, adn, aup)


def solution(mesh):
    placed = (
        P(("grp", "exp"), None),
        P(("grp", "exp"), None),
        P(("grp", "exp"), None),
        P("grp"),
        P("exp", None, None),
        P("exp", None, None),
        P("exp", None, None),
        P("exp", None),
        P("exp", None),
    )
    return jax.shard_map(
        per_device, mesh=mesh, in_specs=placed, out_specs=P(("grp", "exp"), None), check_vma=False
    )
```
